256 devices in a mesh: rows: 64 (over z, y, core), cols: 4 (over x).
Axes of the slice: x: 4, y: 4, z: 8, core: 2. Of those that a mesh axis runs over, the one named last changes fastest.
Arguments:
- gradients: float32 [256, 128, 4096], P(None, 'rows', 'cols'), may hold values from -6 to 6
- momentum: float32 [256, 128, 4096], P(None, 'rows', 'cols'), may hold values from -6 to 6
- weights: float32 [256, 128, 4096], P(None, 'rows', 'cols'), may hold values from -0.1875 to 0.1875
Outputs:
- new_weights: float32 [256, 128, 4096], P(None, 'rows', 'cols')
- new_momentum: float32 [256, 128, 4096], P(None, 'rows', 'cols')
The draws below stay inside these ranges and needn't reach their ends.
All inputs are finite; a program needn't handle non-finite values.
Results may differ from the reference program's by a relative error of at most 0.0003.
Values sent between devices are 32-bit elements.
A program may use at most 64 MiB of HBM per device.

```python
import jax
import jax.numpy as jnp
from jax import lax

SIDE = 128
WIDE = 4096
MATS = 256
ITERS = 4


def level_of(stream_key, dims, pieces, least, largest):
    def one(dim, blocks):
        steps = jax.random.uniform(jax.random.fold_in(jax.random.fold_in(stream_key, 6), dim), (blocks,), jnp.float32, least / len(pieces), largest / len(pieces))
        return jnp.repeat(jnp.exp(steps), dims[dim] // blocks).reshape((-1,) + (1,) * (len(dims) - dim - 1))

    gain = one(*pieces[0])
    for cut in pieces[1:]:
        gain = gain * one(*cut)
    return gain


def noise(stream_key, extent, scale, limit, cuts=(), kind=jnp.bfloat16):
    result = scale * jax.random.normal(stream_key, extent, jnp.float32)
    if cuts:
        result = result * level_of(stream_key, extent, cuts, -0.22, 0.18)
    return jnp.clip(result, -limit, limit).astype(kind)


def setup_inputs(seed: int = 0) -> dict:
    streams_of = jax.random.split(jax.random.key(seed), 4)
    return {
        "gradients": noise(streams_of[0], (MATS, SIDE, WIDE), 1.0, 6.0, ((1, 64), (2, 4)), jnp.float32),
        "momentum": noise(streams_of[1], (MATS, SIDE, WIDE), 1.0, 6.0, ((1, 64), (2, 4)), jnp.float32),
        "weights": noise(streams_of[2], (MATS, SIDE, WIDE), 0.03, 0.1875, ((1, 64), (2, 4)), jnp.float32),
    }


hold_rate = 0.8
learn_rate = 0.8
decay_rate = 0.1

def reference(gradients, momentum, weights):
    new_momentum = hold_rate * momentum + gradients

    def orthogonal_one(stack):
        iterate = stack[None]
        iterate = iterate * lax.rsqrt(lax.optimization_barrier(jnp.sum(iterate * iterate, axis=(1, 2), keepdims=True)) + 1e-06)
        for step in range(ITERS):
            gram = jnp.einsum('mik,mjk->mij', iterate, iterate, precision=lax.Precision.HIGHEST)
            mixed = -4.775 * gram + 2.0315 * jnp.einsum('mij,mjk->mik', gram, gram, precision=lax.Precision.HIGHEST)
            iterate = 3.4445 * iterate + jnp.einsum('mij,mjk->mik', mixed, iterate, precision=lax.Precision.HIGHEST)
        return iterate[0]
    iterate = lax.map(orthogonal_one, new_momentum)
    new_weights = (1.0 - learn_rate * decay_rate) * weights - learn_rate * iterate
    return (new_weights, new_momentum)
```

```python
import jax
import jax.numpy as jnp
from jax import lax
from jax.experimental import pallas as pl
from jax.experimental.pallas import tpu as pltpu
from jax.sharding import PartitionSpec as P

ITERS = 4
GROUPS = 4
Z, Y, CORES = 8, 4, 2
ROWS = Z * Y * CORES
COLS = 4
SIDE = 128
LANES = 128
UNIT = 16
WHOLE = ROWS * UNIT
MESH = pl.DeviceIdType.MESH

hold_rate = 0.8
learn_rate = 0.8
decay_rate = 0.1


def product(a, b, over=0):
    return lax.dot_general(
        a, b, (((1,), (over,)), ((), ())),
        precision=lax.Precision.HIGHEST, preferred_element_type=jnp.float32,
    )


def kernel(x_ref, back_ref, held, grams, done, there_send, there_recv, gram_send, gram_recv, back_send, back_recv):
    r = lax.axis_index("rows")
    c = lax.axis_index("cols")
    z, y, k = r // (Y * CORES), (r // CORES) % Y, r % CORES

    def partner(i):
        return (
            lax.rem(z + i % Z, Z) * (Y * CORES)
            + lax.rem(y + (i // Z) % Y, Y) * CORES
            + lax.rem(k + i // (Z * Y), CORES)
        )

    barrier = pltpu.get_barrier_semaphore()

    def greet(i, carry):
        pl.semaphore_signal(barrier, inc=1, device_id=(partner(i), c), device_id_type=MESH)
        return carry

    lax.fori_loop(1, ROWS, greet, 0)
    for step in range(1, COLS):
        pl.semaphore_signal(barrier, inc=1, device_id=(r, lax.rem(c + step, COLS)), device_id_type=MESH)
    pl.semaphore_wait(barrier, ROWS - 1 + COLS - 1)

    def unit(start):
        return pl.ds(pl.multiple_of(start, UNIT), UNIT)

    for g in range(GROUPS):
        def there(i, carry):
            p = partner(i)
            pltpu.make_async_remote_copy(
                x_ref.at[unit((p * GROUPS + g) * UNIT)],
                held.at[unit(g * WHOLE + r * UNIT)],
                there_send, there_recv.at[g],
                device_id=(p, c), device_id_type=MESH,
            ).start()
            return carry

        lax.fori_loop(1, ROWS, there, 0)
    for g in range(GROUPS):
        held[unit(g * WHOLE + r * UNIT), :] = x_ref[unit((r * GROUPS + g) * UNIT), :]

    row = lax.broadcasted_iota(jnp.int32, (SIDE, SIDE), 0)
    col = lax.broadcasted_iota(jnp.int32, (SIDE, SIDE), 1)
    diagonal = row == col
    half = ROWS
    most = pl.ds(0, (ROWS - 1) * UNIT)

    def rows_of(g):
        return jnp.concatenate(
            [
                jnp.concatenate(
                    [held[pl.ds(g * WHOLE + j * 2 + s, half, stride=UNIT), :] for j in range(UNIT // 2)], axis=1
                )
                for s in range(2)
            ],
            axis=0,
        )

    right = (r, lax.rem(c + 1, COLS))
    for g in range(GROUPS):
        pltpu.make_async_remote_copy(
            x_ref.at[most], held.at[most], there_send, there_recv.at[g], device_id=right, device_id_type=MESH
        ).wait_recv()
        matrix = rows_of(g)
        grams[g, c] = product(matrix, matrix, 1)
        for step in range(1, COLS):
            pltpu.make_async_remote_copy(
                grams.at[g, c], grams.at[g, c], gram_send, gram_recv.at[g],
                device_id=(r, lax.rem(c + step, COLS)), device_id_type=MESH,
            ).start()
        pltpu.make_async_remote_copy(
            grams.at[g, pl.ds(0, COLS - 1)], grams.at[g, pl.ds(0, COLS - 1)], gram_send, gram_recv.at[g],
            device_id=right, device_id_type=MESH,
        ).wait_recv()
        gram = (grams[g, 0] + grams[g, 1]) + (grams[g, 2] + grams[g, 3])
        scale = lax.rsqrt(jnp.sum(jnp.where(diagonal, gram, 0.0), axis=(0, 1), keepdims=True) + 1e-06)
        gram = (gram * scale) * scale
        total = None
        for step in range(ITERS):
            mixed = -4.775 * gram + 2.0315 * product(gram, gram)
            if step == 0:
                total = jnp.where(diagonal, 3.4445, 0.0) + mixed
            else:
                total = 3.4445 * total + product(mixed, total)
            if step < ITERS - 1:
                gram = 3.4445 * gram + product(mixed, gram)
                gram = 3.4445 * gram + product(mixed, gram)
        result = product(total * scale, matrix)
        for s in range(2):
            for j in range(UNIT // 2):
                done[pl.ds(g * WHOLE + j * 2 + s, half, stride=UNIT), :] = result[
                    s * half : (s + 1) * half, j * LANES : (j + 1) * LANES
                ]

        def again(i, carry):
            p = partner(i)
            pltpu.make_async_remote_copy(
                done.at[unit(g * WHOLE + p * UNIT)],
                back_ref.at[unit((r * GROUPS + g) * UNIT)],
                back_send, back_recv,
                device_id=(p, c), device_id_type=MESH,
            ).start()
            return carry

        lax.fori_loop(1, ROWS, again, 0)
        back_ref[unit((r * GROUPS + g) * UNIT), :] = done[unit(g * WHOLE + r * UNIT), :]

    whole = pl.ds(0, (ROWS - 1) * UNIT * GROUPS)
    pltpu.make_async_remote_copy(
        x_ref.at[whole], held.at[whole], there_send, back_recv, device_id=right, device_id_type=MESH
    ).wait()
    pltpu.make_async_remote_copy(
        done.at[whole], back_ref.at[whole], back_send, back_recv, device_id=right, device_id_type=MESH
    ).wait_send()
    sent = grams.at[pl.ds(0, COLS - 1)]
    pltpu.make_async_remote_copy(
        sent, sent, gram_send, back_recv, device_id=right, device_id_type=MESH
    ).wait_send()


def flat(x):
    return x.reshape(256, 2, 8, 128).transpose(0, 2, 1, 3).reshape(4096, 128)


def unflat(x):
    return x.reshape(256, 8, 2, 128).transpose(0, 2, 1, 3).reshape(256, 2, 1024)


def local(gradients, momentum, weights):
    new_momentum = hold_rate * momentum + gradients
    shape = (ROWS * GROUPS * UNIT, LANES)
    back = pl.pallas_call(
        kernel,
        name="orthogonal",
        out_shape=jax.ShapeDtypeStruct(shape, jnp.float32),
        in_specs=[pl.BlockSpec(memory_space=pltpu.VMEM)],
        out_specs=pl.BlockSpec(memory_space=pltpu.VMEM),
        scratch_shapes=[
            pltpu.VMEM(shape, jnp.float32),
            pltpu.VMEM((GROUPS, COLS, SIDE, SIDE), jnp.float32),
            pltpu.VMEM(shape, jnp.float32),
            pltpu.SemaphoreType.DMA,
            pltpu.SemaphoreType.DMA((GROUPS,)),
            pltpu.SemaphoreType.DMA,
            pltpu.SemaphoreType.DMA((GROUPS,)),
            pltpu.SemaphoreType.DMA,
            pltpu.SemaphoreType.DMA,
        ],
        compiler_params=pltpu.CompilerParams(collective_id=0, has_side_effects=True),
    )(flat(new_momentum))
    new_weights = (1.0 - learn_rate * decay_rate) * weights - learn_rate * unflat(back)
    return (new_weights, new_momentum)


def solution(mesh):
    placed = (P(None, "rows", "cols"), P(None, "rows", "cols"), P(None, "rows", "cols"))
    return jax.shard_map(
        local,
        mesh=mesh,
        in_specs=placed,
        out_specs=(P(None, "rows", "cols"), P(None, "rows", "cols")),
        check_vma=False,
    )
```

```python
import jax
import jax.numpy as jnp
from jax import lax
from jax.experimental import pallas as pl
from jax.experimental.pallas import tpu as pltpu
from jax.sharding import PartitionSpec as P

ITERS = 4
GROUPS = 4
Z, Y, CORES = 8, 4, 2
ROWS = Z * Y * CORES
COLS = 4
SIDE = 128
LANES = 128
UNIT = 16
WHOLE = ROWS * UNIT
MESH = pl.DeviceIdType.MESH
VMEM_LIMIT = 24 * 1024 * 1024

hold_rate = 0.8
learn_rate = 0.8
decay_rate = 0.1


def product(a, b, over=0):
    return lax.dot_general(
        a, b, (((1,), (over,)), ((), ())),
        precision=lax.Precision.HIGHEST, preferred_element_type=jnp.float32,
    )


def kernel(
    g_ref, m_ref, w_ref, back_ref, x_ref,
    held, grams, done, g_buf, m_buf, w_buf,
    load_sem, weight_sem, there_send, there_recv, gram_send, gram_recv, back_send, back_recv,
):
    r = lax.axis_index("rows")
    c = lax.axis_index("cols")
    z, y, k = r // (Y * CORES), (r // CORES) % Y, r % CORES

    along_z = [lax.rem(z + dz, Z) * (Y * CORES) for dz in range(Z)]

    def for_partners(act):
        def some(dy, dk, first):
            near = lax.rem(y + dy, Y) * CORES + lax.rem(k + dk, CORES)
            for dz in range(first, Z):
                act(along_z[dz] + near)

        def body(i, carry):
            some(i % Y, i // Y, 0)
            return carry

        some(0, 0, 1)
        lax.fori_loop(1, Y * CORES, body, 0)

    def unit(start):
        return pl.ds(pl.multiple_of(start, UNIT), UNIT)

    def chunk(g):
        return pl.ds(g * WHOLE, WHOLE)

    barrier = pltpu.get_barrier_semaphore()

    loads = []
    for g in range(GROUPS):
        pair = [
            pltpu.make_async_copy(g_ref.at[chunk(g)], g_buf.at[chunk(g)], load_sem.at[0, g]),
            pltpu.make_async_copy(m_ref.at[chunk(g)], m_buf.at[chunk(g)], load_sem.at[1, g]),
        ]
        for copy in pair:
            copy.start()
        loads.append(pair)
    for_partners(lambda p: pl.semaphore_signal(barrier, inc=1, device_id=(p, c), device_id_type=MESH))
    for step in range(1, COLS):
        pl.semaphore_signal(barrier, inc=1, device_id=(r, lax.rem(c + step, COLS)), device_id_type=MESH)

    for g in range(GROUPS):
        for copy in loads[g]:
            copy.wait()
        x_ref[chunk(g), :] = hold_rate * m_buf[chunk(g), :] + g_buf[chunk(g), :]
    pl.semaphore_wait(barrier, ROWS - 1 + COLS - 1)

    for g in range(GROUPS):
        for_partners(
            lambda p: pltpu.make_async_remote_copy(
                x_ref.at[unit((g * ROWS + p) * UNIT)],
                held.at[unit((g * ROWS + r) * UNIT)],
                there_send, there_recv.at[g],
                device_id=(p, c), device_id_type=MESH,
            ).start()
        )
    weights = pltpu.make_async_copy(w_ref, w_buf, weight_sem)
    weights.start()
    for g in range(GROUPS):
        own = unit((g * ROWS + r) * UNIT)
        held[own, :] = x_ref[own, :]

    row = lax.broadcasted_iota(jnp.int32, (SIDE, SIDE), 0)
    col = lax.broadcasted_iota(jnp.int32, (SIDE, SIDE), 1)
    diagonal = row == col
    half = ROWS
    most = pl.ds(0, (ROWS - 1) * UNIT)

    def rows_of(g):
        return jnp.concatenate(
            [
                jnp.concatenate(
                    [held[pl.ds(g * WHOLE + j * 2 + s, half, stride=UNIT), :] for j in range(UNIT // 2)], axis=1
                )
                for s in range(2)
            ],
            axis=0,
        )

    right = (r, lax.rem(c + 1, COLS))
    for g in range(GROUPS):
        pltpu.make_async_remote_copy(
            x_ref.at[most], held.at[most], there_send, there_recv.at[g], device_id=right, device_id_type=MESH
        ).wait_recv()
        matrix = rows_of(g)
        grams[g, c] = product(matrix, matrix, 1)
        for step in range(1, COLS):
            pltpu.make_async_remote_copy(
                grams.at[g, c], grams.at[g, c], gram_send, gram_recv.at[g],
                device_id=(r, lax.rem(c + step, COLS)), device_id_type=MESH,
            ).start()
        pltpu.make_async_remote_copy(
            grams.at[g, pl.ds(0, COLS - 1)], grams.at[g, pl.ds(0, COLS - 1)], gram_send, gram_recv.at[g],
            device_id=right, device_id_type=MESH,
        ).wait_recv()
        gram = (grams[g, 0] + grams[g, 1]) + (grams[g, 2] + grams[g, 3])
        scale = lax.rsqrt(jnp.sum(jnp.where(diagonal, gram, 0.0), axis=(0, 1), keepdims=True) + 1e-06)
        gram = (gram * scale) * scale
        total = None
        for step in range(ITERS):
            mixed = -4.775 * gram + 2.0315 * product(gram, gram)
            if step == 0:
                total = jnp.where(diagonal, 3.4445, 0.0) + mixed
            else:
                total = 3.4445 * total + product(mixed, total)
            if step < ITERS - 1:
                gram = 3.4445 * gram + product(mixed, gram)
                gram = 3.4445 * gram + product(mixed, gram)
        result = product(total * scale, matrix)
        for s in range(2):
            for j in range(UNIT // 2):
                done[pl.ds(g * WHOLE + j * 2 + s, half, stride=UNIT), :] = result[
                    s * half : (s + 1) * half, j * LANES : (j + 1) * LANES
                ]

        for_partners(
            lambda p: pltpu.make_async_remote_copy(
                done.at[unit((g * ROWS + p) * UNIT)],
                back_ref.at[unit((g * ROWS + r) * UNIT)],
                back_send, back_recv.at[g],
                device_id=(p, c), device_id_type=MESH,
            ).start()
        )
        own = unit((g * ROWS + r) * UNIT)
        back_ref[own, :] = done[own, :]

    weights.wait()
    for g in range(GROUPS):
        pltpu.make_async_remote_copy(
            x_ref.at[most], back_ref.at[most], there_send, back_recv.at[g], device_id=right, device_id_type=MESH
        ).wait_recv()
        back_ref[chunk(g), :] = (1.0 - learn_rate * decay_rate) * w_buf[chunk(g), :] - learn_rate * back_ref[chunk(g), :]

    whole = pl.ds(0, (ROWS - 1) * UNIT * GROUPS)
    pltpu.make_async_remote_copy(
        x_ref.at[whole], held.at[whole], there_send, there_recv.at[0], device_id=right, device_id_type=MESH
    ).wait_send()
    pltpu.make_async_remote_copy(
        done.at[whole], back_ref.at[whole], back_send, back_recv.at[0], device_id=right, device_id_type=MESH
    ).wait_send()
    sent = grams.at[pl.ds(0, COLS - 1)]
    pltpu.make_async_remote_copy(
        sent, sent, gram_send, gram_recv.at[0], device_id=right, device_id_type=MESH
    ).wait_send()


def write(weights, momentum, weights_out, momentum_out, sems):
    copies = [
        pltpu.make_async_copy(weights, weights_out, sems.at[0]),
        pltpu.make_async_copy(momentum, momentum_out, sems.at[1]),
    ]
    for copy in copies:
        copy.start()
    for copy in copies:
        copy.wait()


def flat(x):
    return x.reshape(256, 2, 8, 128).transpose(0, 2, 1, 3).reshape(4096, 128)


def unflat(x):
    return x.reshape(256, 8, 2, 128).transpose(0, 2, 1, 3).reshape(256, 2, 1024)


def local(gradients, momentum, weights):
    shape = (ROWS * GROUPS * UNIT, LANES)
    new_weights, new_momentum = pl.pallas_call(
        kernel,
        name="orthogonal",
        out_shape=[jax.ShapeDtypeStruct(shape, jnp.float32)] * 2,
        in_specs=[pl.BlockSpec(memory_space=pltpu.HBM)] * 3,
        out_specs=[pl.BlockSpec(memory_space=pltpu.VMEM)] * 2,
        scratch_shapes=[
            pltpu.VMEM(shape, jnp.float32),
            pltpu.VMEM((GROUPS, COLS, SIDE, SIDE), jnp.float32),
            pltpu.VMEM(shape, jnp.float32),
            pltpu.VMEM(shape, jnp.float32),
            pltpu.VMEM(shape, jnp.float32),
            pltpu.VMEM(shape, jnp.float32),
            pltpu.SemaphoreType.DMA((2, GROUPS)),
            pltpu.SemaphoreType.DMA,
            pltpu.SemaphoreType.DMA,
            pltpu.SemaphoreType.DMA((GROUPS,)),
            pltpu.SemaphoreType.DMA,
            pltpu.SemaphoreType.DMA((GROUPS,)),
            pltpu.SemaphoreType.DMA,
            pltpu.SemaphoreType.DMA((GROUPS,)),
        ],
        compiler_params=pltpu.CompilerParams(collective_id=0, has_side_effects=True, vmem_limit_bytes=VMEM_LIMIT),
    )(*(pltpu.with_memory_space_constraint(flat(x), pltpu.HBM) for x in (gradients, momentum, weights)))
    new_weights, new_momentum = pl.pallas_call(
        write,
        name="write",
        out_shape=[jax.ShapeDtypeStruct(shape, jnp.float32)] * 2,
        in_specs=[pl.BlockSpec(memory_space=pltpu.VMEM)] * 2,
        out_specs=[pl.BlockSpec(memory_space=pltpu.HBM)] * 2,
        scratch_shapes=[pltpu.SemaphoreType.DMA((2,))],
        compiler_params=pltpu.CompilerParams(vmem_limit_bytes=8 * 1024 * 1024),
    )(new_weights, new_momentum)
    return (unflat(new_weights), unflat(new_momentum))


def solution(mesh):
    placed = (P(None, "rows", "cols"), P(None, "rows", "cols"), P(None, "rows", "cols"))
    return jax.shard_map(
        local,
        mesh=mesh,
        in_specs=placed,
        out_specs=(P(None, "rows", "cols"), P(None, "rows", "cols")),
        check_vma=False,
    )
```

```python
import jax
import jax.numpy as jnp
from jax import lax
from jax.experimental import pallas as pl
from jax.experimental.pallas import tpu as pltpu
from jax.sharding import PartitionSpec as P

ITERS = 4
GROUPS = 4
Z, Y, CORES = 8, 4, 2
ROWS = Z * Y * CORES
COLS = 4
SIDE = 128
LANES = 128
UNIT = 16
WHOLE = ROWS * UNIT
MESH = pl.DeviceIdType.MESH
VMEM_LIMIT = 24 * 1024 * 1024

hold_rate = 0.8
learn_rate = 0.8
decay_rate = 0.1


def product(a, b, over=0):
    return lax.dot_general(
        a, b, (((1,), (over,)), ((), ())),
        precision=lax.Precision.HIGHEST, preferred_element_type=jnp.float32,
    )


def kernel(
    g_ref, m_ref, w_ref, back_ref, x_ref,
    held, grams, done, g_buf, m_buf, w_buf,
    here, load_sem, weight_sem, there_send, there_recv, gram_send, gram_recv, back_send, back_recv,
):
    r = lax.axis_index("rows")
    c = lax.axis_index("cols")
    z, y, k = r // (Y * CORES), (r // CORES) % Y, r % CORES

    along_z = [lax.rem(z + dz, Z) * (Y * CORES) for dz in range(Z)]

    def some(act, dy, dk, steps):
        near = lax.rem(y + dy, Y) * CORES + lax.rem(k + dk, CORES)
        for dz in steps:
            act(along_z[dz] + near)

    def for_near(act, steps):
        def body(i, carry):
            some(act, i % Y, i // Y, steps)
            return carry

        some(act, 0, 0, [dz for dz in steps if dz])
        lax.fori_loop(1, Y * CORES, body, 0)

    def for_all(act):
        steps = (4, 5, 3, 6, 2, 7, 1, 0)

        def body(i, carry):
            upper, lower = i // 4, i // 2 % 2
            some(act, 2 + upper - lower - 2 * upper * lower, 1 - i % 2, steps)
            return carry

        lax.fori_loop(0, Y * CORES - 1, body, 0)
        some(act, 0, 0, steps[:-1])

    def unit(start):
        return pl.ds(pl.multiple_of(start, UNIT), UNIT)

    def chunk(g):
        return pl.ds(g * WHOLE, WHOLE)

    barrier = pltpu.get_barrier_semaphore()

    loads = []
    for g in range(GROUPS):
        pair = [
            pltpu.make_async_copy(g_ref.at[chunk(g)], g_buf.at[chunk(g)], load_sem.at[0, g]),
            pltpu.make_async_copy(m_ref.at[chunk(g)], m_buf.at[chunk(g)], load_sem.at[1, g]),
        ]
        for copy in pair:
            copy.start()
        loads.append(pair)
    def signal(semaphore, device):
        pl.semaphore_signal(semaphore, inc=1, device_id=(device, c), device_id_type=MESH)

    for_near(lambda p: signal(barrier, p), (1, 7, 0))
    for step in range(1, COLS):
        pl.semaphore_signal(barrier, inc=1, device_id=(r, lax.rem(c + step, COLS)), device_id_type=MESH)

    def there(g, steps):
        for_near(
            lambda p: pltpu.make_async_remote_copy(
                x_ref.at[unit((g * ROWS + p) * UNIT)],
                held.at[unit((g * ROWS + r) * UNIT)],
                there_send, there_recv.at[g],
                device_id=(p, c), device_id_type=MESH,
            ).start(),
            steps,
        )

    def add(g):
        for copy in loads[g]:
            copy.wait()
        x_ref[chunk(g), :] = hold_rate * m_buf[chunk(g), :] + g_buf[chunk(g), :]

    def tell(stage):
        for dz in (1, Z - 1):
            signal(here.at[stage], along_z[dz] + y * CORES + k)

    add(0)
    pl.semaphore_wait(barrier, 3 * Y * CORES - 1 + COLS - 1)
    tell(0)
    there(0, (1, 7, 0))
    add(1)
    there(1, (1, 7, 0))
    pl.semaphore_wait(here.at[0], 2)
    tell(1)
    there(0, (2, 6))
    pl.semaphore_wait(here.at[1], 2)
    tell(2)
    there(0, (3, 5))
    pl.semaphore_wait(here.at[2], 2)
    there(0, (4,))
    there(1, (2, 6, 3, 5, 4))
    for g in range(2, GROUPS):
        add(g)
        there(g, (1, 7, 2, 6, 3, 5, 4, 0))
    weights = pltpu.make_async_copy(w_ref, w_buf, weight_sem)
    weights.start()
    for g in range(GROUPS):
        own = unit((g * ROWS + r) * UNIT)
        held[own, :] = x_ref[own, :]

    row = lax.broadcasted_iota(jnp.int32, (SIDE, SIDE), 0)
    col = lax.broadcasted_iota(jnp.int32, (SIDE, SIDE), 1)
    diagonal = row == col
    half = ROWS
    most = pl.ds(0, (ROWS - 1) * UNIT)

    def rows_of(g):
        return jnp.concatenate(
            [
                jnp.concatenate(
                    [held[pl.ds(g * WHOLE + j * 2 + s, half, stride=UNIT), :] for j in range(UNIT // 2)], axis=1
                )
                for s in range(2)
            ],
            axis=0,
        )

    right = (r, lax.rem(c + 1, COLS))
    for g in range(GROUPS):
        pltpu.make_async_remote_copy(
            x_ref.at[most], held.at[most], there_send, there_recv.at[g], device_id=right, device_id_type=MESH
        ).wait_recv()
        matrix = rows_of(g)
        grams[g, c] = product(matrix, matrix, 1)
        for step in range(1, COLS):
            pltpu.make_async_remote_copy(
                grams.at[g, c], grams.at[g, c], gram_send, gram_recv.at[g],
                device_id=(r, lax.rem(c + step, COLS)), device_id_type=MESH,
            ).start()
        pltpu.make_async_remote_copy(
            grams.at[g, pl.ds(0, COLS - 1)], grams.at[g, pl.ds(0, COLS - 1)], gram_send, gram_recv.at[g],
            device_id=right, device_id_type=MESH,
        ).wait_recv()
        gram = (grams[g, 0] + grams[g, 1]) + (grams[g, 2] + grams[g, 3])
        scale = lax.rsqrt(jnp.sum(jnp.where(diagonal, gram, 0.0), axis=(0, 1), keepdims=True) + 1e-06)
        gram = (gram * scale) * scale
        total = None
        for step in range(ITERS):
            mixed = -4.775 * gram + 2.0315 * product(gram, gram)
            if step == 0:
                total = jnp.where(diagonal, 3.4445, 0.0) + mixed
            else:
                total = 3.4445 * total + product(mixed, total)
            if step < ITERS - 1:
                gram = 3.4445 * gram + product(mixed, gram)
                gram = 3.4445 * gram + product(mixed, gram)
        result = product(total * scale, matrix)
        for s in range(2):
            for j in range(UNIT // 2):
                done[pl.ds(g * WHOLE + j * 2 + s, half, stride=UNIT), :] = result[
                    s * half : (s + 1) * half, j * LANES : (j + 1) * LANES
                ]

        for_all(
            lambda p: pltpu.make_async_remote_copy(
                done.at[unit((g * ROWS + p) * UNIT)],
                back_ref.at[unit((g * ROWS + r) * UNIT)],
                back_send, back_recv.at[g],
                device_id=(p, c), device_id_type=MESH,
            ).start()
        )
        own = unit((g * ROWS + r) * UNIT)
        back_ref[own, :] = done[own, :]

    weights.wait()
    for g in range(GROUPS):
        pltpu.make_async_remote_copy(
            x_ref.at[most], back_ref.at[most], there_send, back_recv.at[g], device_id=right, device_id_type=MESH
        ).wait_recv()
        back_ref[chunk(g), :] = (1.0 - learn_rate * decay_rate) * w_buf[chunk(g), :] - learn_rate * back_ref[chunk(g), :]

    whole = pl.ds(0, (ROWS - 1) * UNIT * GROUPS)
    pltpu.make_async_remote_copy(
        x_ref.at[whole], held.at[whole], there_send, there_recv.at[0], device_id=right, device_id_type=MESH
    ).wait_send()
    pltpu.make_async_remote_copy(
        done.at[whole], back_ref.at[whole], back_send, back_recv.at[0], device_id=right, device_id_type=MESH
    ).wait_send()
    sent = grams.at[pl.ds(0, COLS - 1)]
    pltpu.make_async_remote_copy(
        sent, sent, gram_send, gram_recv.at[0], device_id=right, device_id_type=MESH
    ).wait_send()


def write(weights, momentum, weights_out, momentum_out, sems):
    copies = [
        pltpu.make_async_copy(weights, weights_out, sems.at[0]),
        pltpu.make_async_copy(momentum, momentum_out, sems.at[1]),
    ]
    for copy in copies:
        copy.start()
    for copy in copies:
        copy.wait()


def flat(x):
    return x.reshape(256, 2, 8, 128).transpose(0, 2, 1, 3).reshape(4096, 128)


def unflat(x):
    return x.reshape(256, 8, 2, 128).transpose(0, 2, 1, 3).reshape(256, 2, 1024)


def local(gradients, momentum, weights):
    shape = (ROWS * GROUPS * UNIT, LANES)
    new_weights, new_momentum = pl.pallas_call(
        kernel,
        name="orthogonal",
        out_shape=[jax.ShapeDtypeStruct(shape, jnp.float32)] * 2,
        in_specs=[pl.BlockSpec(memory_space=pltpu.HBM)] * 3,
        out_specs=[pl.BlockSpec(memory_space=pltpu.VMEM)] * 2,
        scratch_shapes=[
            pltpu.VMEM(shape, jnp.float32),
            pltpu.VMEM((GROUPS, COLS, SIDE, SIDE), jnp.float32),
            pltpu.VMEM(shape, jnp.float32),
            pltpu.VMEM(shape, jnp.float32),
            pltpu.VMEM(shape, jnp.float32),
            pltpu.VMEM(shape, jnp.float32),
            pltpu.SemaphoreType.REGULAR((3,)),
            pltpu.SemaphoreType.DMA((2, GROUPS)),
            pltpu.SemaphoreType.DMA,
            pltpu.SemaphoreType.DMA,
            pltpu.SemaphoreType.DMA((GROUPS,)),
            pltpu.SemaphoreType.DMA,
            pltpu.SemaphoreType.DMA((GROUPS,)),
            pltpu.SemaphoreType.DMA,
            pltpu.SemaphoreType.DMA((GROUPS,)),
        ],
        compiler_params=pltpu.CompilerParams(collective_id=0, has_side_effects=True, vmem_limit_bytes=VMEM_LIMIT),
    )(*(pltpu.with_memory_space_constraint(flat(x), pltpu.HBM) for x in (gradients, momentum, weights)))
    new_weights, new_momentum = pl.pallas_call(
        write,
        name="write",
        out_shape=[jax.ShapeDtypeStruct(shape, jnp.float32)] * 2,
        in_specs=[pl.BlockSpec(memory_space=pltpu.VMEM)] * 2,
        out_specs=[pl.BlockSpec(memory_space=pltpu.HBM)] * 2,
        scratch_shapes=[pltpu.SemaphoreType.DMA((2,))],
        compiler_params=pltpu.CompilerParams(vmem_limit_bytes=8 * 1024 * 1024),
    )(new_weights, new_momentum)
    return (unflat(new_weights), unflat(new_momentum))


def solution(mesh):
    placed = (P(None, "rows", "cols"), P(None, "rows", "cols"), P(None, "rows", "cols"))
    return jax.shard_map(
        local,
        mesh=mesh,
        in_specs=placed,
        out_specs=(P(None, "rows", "cols"), P(None, "rows", "cols")),
        check_vma=False,
    )
```

```python
import jax
import jax.numpy as jnp
from jax import lax
from jax.experimental import pallas as pl
from jax.experimental.pallas import tpu as pltpu
from jax.sharding import PartitionSpec as P

ITERS = 4
GROUPS = 4
Z, Y, CORES = 8, 4, 2
ROWS = Z * Y * CORES
COLS = 4
SIDE = 128
LANES = 128
UNIT = 16
WHOLE = ROWS * UNIT
MESH = pl.DeviceIdType.MESH
EARLY_Z = (0, 4, 1, 5, 2, 6, 3, 7)
VMEM_LIMIT = 24 * 1024 * 1024

hold_rate = 0.8
learn_rate = 0.8
decay_rate = 0.1


def product(a, b, over=0):
    return lax.dot_general(
        a, b, (((1,), (over,)), ((), ())),
        precision=lax.Precision.HIGHEST, preferred_element_type=jnp.float32,
    )


def kernel(
    g_ref, m_ref, w_ref, back_ref, x_ref,
    held, grams, done, g_buf, m_buf, w_buf,
    here, load_sem, weight_sem, there_send, there_recv, gram_send, gram_recv, back_send, back_recv,
):
    r = lax.axis_index("rows")
    c = lax.axis_index("cols")
    z, y, k = r // (Y * CORES), (r // CORES) % Y, r % CORES

    along_z = [lax.rem(z + dz, Z) * (Y * CORES) for dz in range(Z)]

    def some(act, dy, dk, steps):
        near = lax.rem(y + dy, Y) * CORES + lax.rem(k + dk, CORES)
        for dz in steps:
            act(along_z[dz] + near)

    def for_near(act, steps):
        def body(i, carry):
            some(act, i % Y, i // Y, steps)
            return carry

        some(act, 0, 0, [dz for dz in steps if dz])
        lax.fori_loop(1, Y * CORES, body, 0)

    def for_all(act, level=0):
        steps = (4, 5, 3, 6, 2, 7, 1, 0)

        def body(i, carry):
            upper, lower = i // 4, i // 2 % 2
            some(act, 2 + upper - lower - 2 * upper * lower, 1 - i % 2, steps)
            return carry

        lax.fori_loop(0, Y * CORES - max(level, 1), body, 0)
        if not level:
            some(act, 0, 0, steps[:-1])
            return
        lasts = [(2, 1), (2, 0), (1, 1), (1, 0), (3, 1), (3, 0), (0, 1), (0, 0)][-level:]
        near = [lax.rem(y + dy, Y) * CORES + lax.rem(k + dk, CORES) for dy, dk in lasts]
        for there_z in EARLY_Z:
            for last, (dy, dk) in zip(near, lasts):
                device = there_z * (Y * CORES) + last
                if (dy, dk) == (0, 0):
                    pl.when(device != r)(lambda device=device: act(device))
                else:
                    act(device)

    def unit(start):
        return pl.ds(pl.multiple_of(start, UNIT), UNIT)

    def chunk(g):
        return pl.ds(g * WHOLE, WHOLE)

    barrier = pltpu.get_barrier_semaphore()

    loads = []
    for g in range(GROUPS):
        pair = [
            pltpu.make_async_copy(g_ref.at[chunk(g)], g_buf.at[chunk(g)], load_sem.at[0, g]),
            pltpu.make_async_copy(m_ref.at[chunk(g)], m_buf.at[chunk(g)], load_sem.at[1, g]),
        ]
        for copy in pair:
            copy.start()
        loads.append(pair)
    def signal(semaphore, device):
        pl.semaphore_signal(semaphore, inc=1, device_id=(device, c), device_id_type=MESH)

    for_near(lambda p: signal(barrier, p), (1, 7, 0))
    for step in range(1, COLS):
        pl.semaphore_signal(barrier, inc=1, device_id=(r, lax.rem(c + step, COLS)), device_id_type=MESH)

    def there(g, steps):
        for_near(
            lambda p: pltpu.make_async_remote_copy(
                x_ref.at[unit((g * ROWS + p) * UNIT)],
                held.at[unit((g * ROWS + r) * UNIT)],
                there_send, there_recv.at[g],
                device_id=(p, c), device_id_type=MESH,
            ).start(),
            steps,
        )

    def add(g):
        for copy in loads[g]:
            copy.wait()
        x_ref[chunk(g), :] = hold_rate * m_buf[chunk(g), :] + g_buf[chunk(g), :]

    def tell(stage):
        for dz in (1, Z - 1):
            signal(here.at[stage], along_z[dz] + y * CORES + k)

    add(0)
    pl.semaphore_wait(barrier, 3 * Y * CORES - 1 + COLS - 1)
    tell(0)
    there(0, (1, 7, 0))
    add(1)
    there(1, (1, 7, 0))
    pl.semaphore_wait(here.at[0], 2)
    tell(1)
    there(0, (2, 6))
    pl.semaphore_wait(here.at[1], 2)
    tell(2)
    there(0, (3, 5))
    pl.semaphore_wait(here.at[2], 2)
    there(0, (4,))
    there(1, (2, 6, 3, 5, 4))
    for g in range(2, GROUPS):
        add(g)
        there(g, (1, 7, 2, 6, 3, 5, 4, 0))
    weights = pltpu.make_async_copy(w_ref, w_buf, weight_sem)
    weights.start()
    for g in range(GROUPS):
        own = unit((g * ROWS + r) * UNIT)
        held[own, :] = x_ref[own, :]

    row = lax.broadcasted_iota(jnp.int32, (SIDE, SIDE), 0)
    col = lax.broadcasted_iota(jnp.int32, (SIDE, SIDE), 1)
    diagonal = row == col
    half = ROWS
    most = pl.ds(0, (ROWS - 1) * UNIT)

    def rows_of(g):
        return jnp.concatenate(
            [
                jnp.concatenate(
                    [held[pl.ds(g * WHOLE + j * 2 + s, half, stride=UNIT), :] for j in range(UNIT // 2)], axis=1
                )
                for s in range(2)
            ],
            axis=0,
        )

    right = (r, lax.rem(c + 1, COLS))
    for g in range(GROUPS):
        pltpu.make_async_remote_copy(
            x_ref.at[most], held.at[most], there_send, there_recv.at[g], device_id=right, device_id_type=MESH
        ).wait_recv()
        matrix = rows_of(g)
        grams[g, c] = product(matrix, matrix, 1)
        for step in range(1, COLS):
            pltpu.make_async_remote_copy(
                grams.at[g, c], grams.at[g, c], gram_send, gram_recv.at[g],
                device_id=(r, lax.rem(c + step, COLS)), device_id_type=MESH,
            ).start()
        pltpu.make_async_remote_copy(
            grams.at[g, pl.ds(0, COLS - 1)], grams.at[g, pl.ds(0, COLS - 1)], gram_send, gram_recv.at[g],
            device_id=right, device_id_type=MESH,
        ).wait_recv()
        gram = (grams[g, 0] + grams[g, 1]) + (grams[g, 2] + grams[g, 3])
        scale = lax.rsqrt(jnp.sum(jnp.where(diagonal, gram, 0.0), axis=(0, 1), keepdims=True) + 1e-06)
        gram = (gram * scale) * scale
        total = None
        for step in range(ITERS):
            mixed = -4.775 * gram + 2.0315 * product(gram, gram)
            if step == 0:
                total = jnp.where(diagonal, 3.4445, 0.0) + mixed
            else:
                total = 3.4445 * total + product(mixed, total)
            if step < ITERS - 1:
                gram = 3.4445 * gram + product(mixed, gram)
                gram = 3.4445 * gram + product(mixed, gram)
        result = product(total * scale, matrix)
        for s in range(2):
            for j in range(UNIT // 2):
                done[pl.ds(g * WHOLE + j * 2 + s, half, stride=UNIT), :] = result[
                    s * half : (s + 1) * half, j * LANES : (j + 1) * LANES
                ]

        for_all(
            lambda p: pltpu.make_async_remote_copy(
                done.at[unit((g * ROWS + p) * UNIT)],
                back_ref.at[unit((g * ROWS + r) * UNIT)],
                back_send, back_recv.at[g],
                device_id=(p, c), device_id_type=MESH,
            ).start(),
            4 if g == GROUPS - 1 else 0,
        )
        own = unit((g * ROWS + r) * UNIT)
        back_ref[own, :] = done[own, :]

    weights.wait()
    for g in range(GROUPS):
        pltpu.make_async_remote_copy(
            x_ref.at[most], back_ref.at[most], there_send, back_recv.at[g], device_id=right, device_id_type=MESH
        ).wait_recv()
        back_ref[chunk(g), :] = (1.0 - learn_rate * decay_rate) * w_buf[chunk(g), :] - learn_rate * back_ref[chunk(g), :]

    whole = pl.ds(0, (ROWS - 1) * UNIT * GROUPS)
    pltpu.make_async_remote_copy(
        x_ref.at[whole], held.at[whole], there_send, there_recv.at[0], device_id=right, device_id_type=MESH
    ).wait_send()
    pltpu.make_async_remote_copy(
        done.at[whole], back_ref.at[whole], back_send, back_recv.at[0], device_id=right, device_id_type=MESH
    ).wait_send()
    sent = grams.at[pl.ds(0, COLS - 1)]
    pltpu.make_async_remote_copy(
        sent, sent, gram_send, gram_recv.at[0], device_id=right, device_id_type=MESH
    ).wait_send()


def write(weights, momentum, weights_out, momentum_out, sems):
    copies = [
        pltpu.make_async_copy(weights, weights_out, sems.at[0]),
        pltpu.make_async_copy(momentum, momentum_out, sems.at[1]),
    ]
    for copy in copies:
        copy.start()
    for copy in copies:
        copy.wait()


def flat(x):
    return x.reshape(256, 2, 8, 128).transpose(0, 2, 1, 3).reshape(4096, 128)


def unflat(x):
    return x.reshape(256, 8, 2, 128).transpose(0, 2, 1, 3).reshape(256, 2, 1024)


def local(gradients, momentum, weights):
    shape = (ROWS * GROUPS * UNIT, LANES)
    new_weights, new_momentum = pl.pallas_call(
        kernel,
        name="orthogonal",
        out_shape=[jax.ShapeDtypeStruct(shape, jnp.float32)] * 2,
        in_specs=[pl.BlockSpec(memory_space=pltpu.HBM)] * 3,
        out_specs=[pl.BlockSpec(memory_space=pltpu.VMEM)] * 2,
        scratch_shapes=[
            pltpu.VMEM(shape, jnp.float32),
            pltpu.VMEM((GROUPS, COLS, SIDE, SIDE), jnp.float32),
            pltpu.VMEM(shape, jnp.float32),
            pltpu.VMEM(shape, jnp.float32),
            pltpu.VMEM(shape, jnp.float32),
            pltpu.VMEM(shape, jnp.float32),
            pltpu.SemaphoreType.REGULAR((3,)),
            pltpu.SemaphoreType.DMA((2, GROUPS)),
            pltpu.SemaphoreType.DMA,
            pltpu.SemaphoreType.DMA,
            pltpu.SemaphoreType.DMA((GROUPS,)),
            pltpu.SemaphoreType.DMA,
            pltpu.SemaphoreType.DMA((GROUPS,)),
            pltpu.SemaphoreType.DMA,
            pltpu.SemaphoreType.DMA((GROUPS,)),
        ],
        compiler_params=pltpu.CompilerParams(collective_id=0, has_side_effects=True, vmem_limit_bytes=VMEM_LIMIT),
    )(*(pltpu.with_memory_space_constraint(flat(x), pltpu.HBM) for x in (gradients, momentum, weights)))
    new_weights, new_momentum = pl.pallas_call(
        write,
        name="write",
        out_shape=[jax.ShapeDtypeStruct(shape, jnp.float32)] * 2,
        in_specs=[pl.BlockSpec(memory_space=pltpu.VMEM)] * 2,
        out_specs=[pl.BlockSpec(memory_space=pltpu.HBM)] * 2,
        scratch_shapes=[pltpu.SemaphoreType.DMA((2,))],
        compiler_params=pltpu.CompilerParams(vmem_limit_bytes=8 * 1024 * 1024),
    )(new_weights, new_momentum)
    return (unflat(new_weights), unflat(new_momentum))


def solution(mesh):
    placed = (P(None, "rows", "cols"), P(None, "rows", "cols"), P(None, "rows", "cols"))
    return jax.shard_map(
        local,
        mesh=mesh,
        in_specs=placed,
        out_specs=(P(None, "rows", "cols"), P(None, "rows", "cols")),
        check_vma=False,
    )
```

```python
import jax
import jax.numpy as jnp
from jax import lax
from jax.experimental import pallas as pl
from jax.experimental.pallas import tpu as pltpu
from jax.sharding import PartitionSpec as P

ITERS = 4
GROUPS = 4
Z, Y, CORES = 8, 4, 2
ROWS = Z * Y * CORES
COLS = 4
SIDE = 128
LANES = 128
UNIT = 16
WHOLE = ROWS * UNIT
MESH = pl.DeviceIdType.MESH
EARLY_Z = (0, 4, 1, 5, 2, 6, 3, 7)
VMEM_LIMIT = 24 * 1024 * 1024

hold_rate = 0.8
learn_rate = 0.8
decay_rate = 0.1


def product(a, b, over=0):
    return lax.dot_general(
        a, b, (((1,), (over,)), ((), ())),
        precision=lax.Precision.HIGHEST, preferred_element_type=jnp.float32,
    )


def kernel(
    g_ref, m_ref, w_ref, back_ref, x_ref,
    held, grams, done, g_buf, m_buf, w_buf,
    here, load_sem, weight_sem, there_send, there_recv, gram_send, gram_recv, back_send, back_recv,
):
    r = lax.axis_index("rows")
    c = lax.axis_index("cols")
    z, y, k = r // (Y * CORES), (r // CORES) % Y, r % CORES

    along_z = [lax.rem(z + dz, Z) * (Y * CORES) for dz in range(Z)]

    def some(act, dy, dk, steps):
        near = lax.rem(y + dy, Y) * CORES + lax.rem(k + dk, CORES)
        for dz in steps:
            act(along_z[dz] + near)

    def for_near(act, steps):
        def body(i, carry):
            some(act, i % Y, i // Y, steps)
            return carry

        some(act, 0, 0, [dz for dz in steps if dz])
        lax.fori_loop(1, Y * CORES, body, 0)

    def for_all(act, level=0):
        steps = (4, 5, 3, 6, 2, 7, 1, 0)

        def body(i, carry):
            upper, lower = i // 4, i // 2 % 2
            some(act, 2 + upper - lower - 2 * upper * lower, 1 - i % 2, steps)
            return carry

        lax.fori_loop(0, Y * CORES - max(level, 1), body, 0)
        if not level:
            some(act, 0, 0, steps[:-1])
            return
        lasts = [(2, 1), (2, 0), (1, 1), (1, 0), (3, 1), (3, 0), (0, 1), (0, 0)][-level:]
        near = [lax.rem(y + dy, Y) * CORES + lax.rem(k + dk, CORES) for dy, dk in lasts]
        for there_z in EARLY_Z:
            for last, (dy, dk) in zip(near, lasts):
                device = there_z * (Y * CORES) + last
                if (dy, dk) == (0, 0):
                    pl.when(device != r)(lambda device=device: act(device))
                else:
                    act(device)

    def unit(start):
        return pl.ds(pl.multiple_of(start, UNIT), UNIT)

    def chunk(g):
        return pl.ds(g * WHOLE, WHOLE)

    barrier = pltpu.get_barrier_semaphore()

    def signal(semaphore, device):
        pl.semaphore_signal(semaphore, inc=1, device_id=(device, c), device_id_type=MESH)

    for step in (2, 1, 3):
        pl.semaphore_signal(barrier, inc=1, device_id=(r, lax.rem(c + step, COLS)), device_id_type=MESH)
    for dy in (2, 1, 3, 0):
        for dk in (1, 0):
            some(lambda p: signal(barrier, p), dy, dk, (1, 7, 0) if dy or dk else (1, 7))

    loads = []
    for g in range(GROUPS):
        pair = [
            pltpu.make_async_copy(g_ref.at[chunk(g)], g_buf.at[chunk(g)], load_sem.at[0, g]),
            pltpu.make_async_copy(m_ref.at[chunk(g)], m_buf.at[chunk(g)], load_sem.at[1, g]),
        ]
        for copy in pair:
            copy.start()
        loads.append(pair)

    def there(g, steps):
        for_near(
            lambda p: pltpu.make_async_remote_copy(
                x_ref.at[unit((g * ROWS + p) * UNIT)],
                held.at[unit((g * ROWS + r) * UNIT)],
                there_send, there_recv.at[g],
                device_id=(p, c), device_id_type=MESH,
            ).start(),
            steps,
        )

    def add(g):
        for copy in loads[g]:
            copy.wait()
        x_ref[chunk(g), :] = hold_rate * m_buf[chunk(g), :] + g_buf[chunk(g), :]

    def tell(stage):
        for dz in (1, Z - 1):
            signal(here.at[stage], along_z[dz] + y * CORES + k)

    add(0)
    pl.semaphore_wait(barrier, 3 * Y * CORES - 1 + COLS - 1)
    tell(0)
    there(0, (1, 7, 0))
    add(1)
    there(1, (1, 7, 0))
    pl.semaphore_wait(here.at[0], 2)
    tell(1)
    there(0, (2, 6))
    pl.semaphore_wait(here.at[1], 2)
    tell(2)
    there(0, (3, 5))
    pl.semaphore_wait(here.at[2], 2)
    there(0, (4,))
    there(1, (2, 6, 3, 5, 4))
    for g in range(2, GROUPS):
        add(g)
        there(g, (1, 7, 2, 6, 3, 5, 4, 0))
    weights = pltpu.make_async_copy(w_ref, w_buf, weight_sem)
    weights.start()
    for g in range(GROUPS):
        own = unit((g * ROWS + r) * UNIT)
        held[own, :] = x_ref[own, :]

    row = lax.broadcasted_iota(jnp.int32, (SIDE, SIDE), 0)
    col = lax.broadcasted_iota(jnp.int32, (SIDE, SIDE), 1)
    diagonal = row == col
    half = ROWS
    most = pl.ds(0, (ROWS - 1) * UNIT)

    def rows_of(g):
        return jnp.concatenate(
            [
                jnp.concatenate(
                    [held[pl.ds(g * WHOLE + j * 2 + s, half, stride=UNIT), :] for j in range(UNIT // 2)], axis=1
                )
                for s in range(2)
            ],
            axis=0,
        )

    right = (r, lax.rem(c + 1, COLS))
    for g in range(GROUPS):
        pltpu.make_async_remote_copy(
            x_ref.at[most], held.at[most], there_send, there_recv.at[g], device_id=right, device_id_type=MESH
        ).wait_recv()
        matrix = rows_of(g)
        grams[g, c] = product(matrix, matrix, 1)
        for step in range(1, COLS):
            pltpu.make_async_remote_copy(
                grams.at[g, c], grams.at[g, c], gram_send, gram_recv.at[g],
                device_id=(r, lax.rem(c + step, COLS)), device_id_type=MESH,
            ).start()
        pltpu.make_async_remote_copy(
            grams.at[g, pl.ds(0, COLS - 1)], grams.at[g, pl.ds(0, COLS - 1)], gram_send, gram_recv.at[g],
            device_id=right, device_id_type=MESH,
        ).wait_recv()
        gram = (grams[g, 0] + grams[g, 1]) + (grams[g, 2] + grams[g, 3])
        scale = lax.rsqrt(jnp.sum(jnp.where(diagonal, gram, 0.0), axis=(0, 1), keepdims=True) + 1e-06)
        gram = (gram * scale) * scale
        total = None
        for step in range(ITERS):
            mixed = -4.775 * gram + 2.0315 * product(gram, gram)
            if step == 0:
                total = jnp.where(diagonal, 3.4445, 0.0) + mixed
            else:
                total = 3.4445 * total + product(mixed, total)
            if step < ITERS - 1:
                gram = 3.4445 * gram + product(mixed, gram)
                gram = 3.4445 * gram + product(mixed, gram)
        result = product(total * scale, matrix)
        for s in range(2):
            for j in range(UNIT // 2):
                done[pl.ds(g * WHOLE + j * 2 + s, half, stride=UNIT), :] = result[
                    s * half : (s + 1) * half, j * LANES : (j + 1) * LANES
                ]

        for_all(
            lambda p: pltpu.make_async_remote_copy(
                done.at[unit((g * ROWS + p) * UNIT)],
                back_ref.at[unit((g * ROWS + r) * UNIT)],
                back_send, back_recv.at[g],
                device_id=(p, c), device_id_type=MESH,
            ).start(),
            4 if g == GROUPS - 1 else 0,
        )
        own = unit((g * ROWS + r) * UNIT)
        back_ref[own, :] = done[own, :]

    whole = pl.ds(0, (ROWS - 1) * UNIT * GROUPS)
    pltpu.make_async_remote_copy(
        x_ref.at[whole], held.at[whole], there_send, there_recv.at[0], device_id=right, device_id_type=MESH
    ).wait_send()
    sent = grams.at[pl.ds(0, COLS - 1)]
    pltpu.make_async_remote_copy(
        sent, sent, gram_send, gram_recv.at[0], device_id=right, device_id_type=MESH
    ).wait_send()
    weights.wait()
    for g in range(GROUPS):
        pltpu.make_async_remote_copy(
            x_ref.at[most], back_ref.at[most], there_send, back_recv.at[g], device_id=right, device_id_type=MESH
        ).wait_recv()
        back_ref[chunk(g), :] = (1.0 - learn_rate * decay_rate) * w_buf[chunk(g), :] - learn_rate * back_ref[chunk(g), :]

    pltpu.make_async_remote_copy(
        done.at[whole], back_ref.at[whole], back_send, back_recv.at[0], device_id=right, device_id_type=MESH
    ).wait_send()


def write(weights, momentum, weights_out, momentum_out, sems):
    copies = [
        pltpu.make_async_copy(weights, weights_out, sems.at[0]),
        pltpu.make_async_copy(momentum, momentum_out, sems.at[1]),
    ]
    for copy in copies:
        copy.start()
    for copy in copies:
        copy.wait()


def flat(x):
    return x.reshape(256, 2, 8, 128).transpose(0, 2, 1, 3).reshape(4096, 128)


def unflat(x):
    return x.reshape(256, 8, 2, 128).transpose(0, 2, 1, 3).reshape(256, 2, 1024)


def local(gradients, momentum, weights):
    shape = (ROWS * GROUPS * UNIT, LANES)
    new_weights, new_momentum = pl.pallas_call(
        kernel,
        name="orthogonal",
        out_shape=[jax.ShapeDtypeStruct(shape, jnp.float32)] * 2,
        in_specs=[pl.BlockSpec(memory_space=pltpu.HBM)] * 3,
        out_specs=[pl.BlockSpec(memory_space=pltpu.VMEM)] * 2,
        scratch_shapes=[
            pltpu.VMEM(shape, jnp.float32),
            pltpu.VMEM((GROUPS, COLS, SIDE, SIDE), jnp.float32),
            pltpu.VMEM(shape, jnp.float32),
            pltpu.VMEM(shape, jnp.float32),
            pltpu.VMEM(shape, jnp.float32),
            pltpu.VMEM(shape, jnp.float32),
            pltpu.SemaphoreType.REGULAR((3,)),
            pltpu.SemaphoreType.DMA((2, GROUPS)),
            pltpu.SemaphoreType.DMA,
            pltpu.SemaphoreType.DMA,
            pltpu.SemaphoreType.DMA((GROUPS,)),
            pltpu.SemaphoreType.DMA,
            pltpu.SemaphoreType.DMA((GROUPS,)),
            pltpu.SemaphoreType.DMA,
            pltpu.SemaphoreType.DMA((GROUPS,)),
        ],
        compiler_params=pltpu.CompilerParams(collective_id=0, has_side_effects=True, vmem_limit_bytes=VMEM_LIMIT),
    )(*(pltpu.with_memory_space_constraint(flat(x), pltpu.HBM) for x in (gradients, momentum, weights)))
    new_weights, new_momentum = pl.pallas_call(
        write,
        name="write",
        out_shape=[jax.ShapeDtypeStruct(shape, jnp.float32)] * 2,
        in_specs=[pl.BlockSpec(memory_space=pltpu.VMEM)] * 2,
        out_specs=[pl.BlockSpec(memory_space=pltpu.HBM)] * 2,
        scratch_shapes=[pltpu.SemaphoreType.DMA((2,))],
        compiler_params=pltpu.CompilerParams(vmem_limit_bytes=8 * 1024 * 1024),
    )(new_weights, new_momentum)
    return (unflat(new_weights), unflat(new_momentum))


def solution(mesh):
    placed = (P(None, "rows", "cols"), P(None, "rows", "cols"), P(None, "rows", "cols"))
    return jax.shard_map(
        local,
        mesh=mesh,
        in_specs=placed,
        out_specs=(P(None, "rows", "cols"), P(None, "rows", "cols")),
        check_vma=False,
    )
```

```python
import jax
import jax.numpy as jnp
from jax import lax
from jax.experimental import pallas as pl
from jax.experimental.pallas import tpu as pltpu
from jax.sharding import PartitionSpec as P

ITERS = 4
GROUPS = 4
Z, Y, CORES = 8, 4, 2
ROWS = Z * Y * CORES
COLS = 4
SIDE = 128
LANES = 128
UNIT = 16
WHOLE = ROWS * UNIT
MESH = pl.DeviceIdType.MESH
EARLY_Z = (0, 4, 1, 5, 2, 6, 3, 7)
VMEM_LIMIT = 24 * 1024 * 1024

hold_rate = 0.8
learn_rate = 0.8
decay_rate = 0.1


def product(a, b, over=0):
    return lax.dot_general(
        a, b, (((1,), (over,)), ((), ())),
        precision=lax.Precision.HIGHEST, preferred_element_type=jnp.float32,
    )


def kernel(
    g_ref, m_ref, w_ref, back_ref, x_ref,
    held, grams, done, g_buf, m_buf, w_buf,
    here, load_sem, weight_sem, there_send, there_recv, gram_send, gram_recv, back_send, back_recv,
):
    r = lax.axis_index("rows")
    c = lax.axis_index("cols")
    z, y, k = r // (Y * CORES), (r // CORES) % Y, r % CORES

    along_z = [lax.rem(z + dz, Z) * (Y * CORES) for dz in range(Z)]

    def some(act, dy, dk, steps):
        near = lax.rem(y + dy, Y) * CORES + lax.rem(k + dk, CORES)
        for dz in steps:
            act(along_z[dz] + near)

    def for_near(act, steps):
        def body(i, carry):
            some(act, i % Y, i // Y, steps)
            return carry

        some(act, 0, 0, [dz for dz in steps if dz])
        lax.fori_loop(1, Y * CORES, body, 0)

    def for_all(act, last=False):
        steps = (4, 5, 3, 6, 2, 7, 1, 0)

        def body(i, carry):
            upper, lower = i // 4, i // 2 % 2
            some(act, 2 + upper - lower - 2 * upper * lower, 1 - i % 2, steps)
            return carry

        def others(device):
            pl.when(device != r)(lambda: act(device))

        def low(i, carry):
            for dz in steps:
                others(along_z[dz] + i)
            return carry

        if last:
            lax.fori_loop(0, CORES, low, 0)
            for there_z in EARLY_Z:
                for near in range(CORES, Y * CORES):
                    others(there_z * (Y * CORES) + near)
        else:
            lax.fori_loop(0, Y * CORES - 1, body, 0)
            some(act, 0, 0, steps[:-1])

    def unit(start):
        return pl.ds(pl.multiple_of(start, UNIT), UNIT)

    def chunk(g):
        return pl.ds(g * WHOLE, WHOLE)

    barrier = pltpu.get_barrier_semaphore()

    loads = []
    for g in range(GROUPS):
        pair = [
            pltpu.make_async_copy(g_ref.at[chunk(g)], g_buf.at[chunk(g)], load_sem.at[0, g]),
            pltpu.make_async_copy(m_ref.at[chunk(g)], m_buf.at[chunk(g)], load_sem.at[1, g]),
        ]
        for copy in pair:
            copy.start()
        loads.append(pair)
    def signal(semaphore, device):
        pl.semaphore_signal(semaphore, inc=1, device_id=(device, c), device_id_type=MESH)

    for_near(lambda p: signal(barrier, p), (1, 7, 0))
    for step in range(1, COLS):
        pl.semaphore_signal(barrier, inc=1, device_id=(r, lax.rem(c + step, COLS)), device_id_type=MESH)

    def there(g, steps):
        for_near(
            lambda p: pltpu.make_async_remote_copy(
                x_ref.at[unit((g * ROWS + p) * UNIT)],
                held.at[unit((g * ROWS + r) * UNIT)],
                there_send, there_recv.at[g],
                device_id=(p, c), device_id_type=MESH,
            ).start(),
            steps,
        )

    def add(g):
        for copy in loads[g]:
            copy.wait()
        x_ref[chunk(g), :] = hold_rate * m_buf[chunk(g), :] + g_buf[chunk(g), :]

    def tell(stage):
        for dz in (1, Z - 1):
            signal(here.at[stage], along_z[dz] + y * CORES + k)

    add(0)
    pl.semaphore_wait(barrier, 3 * Y * CORES - 1 + COLS - 1)
    tell(0)
    there(0, (1, 7, 0))
    add(1)
    there(1, (1, 7, 0))
    pl.semaphore_wait(here.at[0], 2)
    tell(1)
    there(0, (2, 6))
    pl.semaphore_wait(here.at[1], 2)
    tell(2)
    there(0, (3, 5))
    pl.semaphore_wait(here.at[2], 2)
    there(0, (4,))
    there(1, (2, 6, 3, 5, 4))
    for g in range(2, GROUPS):
        add(g)
        there(g, (1, 7, 2, 6, 3, 5, 4, 0))
    weights = pltpu.make_async_copy(w_ref, w_buf, weight_sem)
    weights.start()
    for g in range(GROUPS):
        own = unit((g * ROWS + r) * UNIT)
        held[own, :] = x_ref[own, :]

    row = lax.broadcasted_iota(jnp.int32, (SIDE, SIDE), 0)
    col = lax.broadcasted_iota(jnp.int32, (SIDE, SIDE), 1)
    diagonal = row == col
    half = ROWS
    most = pl.ds(0, (ROWS - 1) * UNIT)

    def rows_of(g):
        return jnp.concatenate(
            [
                jnp.concatenate(
                    [held[pl.ds(g * WHOLE + j * 2 + s, half, stride=UNIT), :] for j in range(UNIT // 2)], axis=1
                )
                for s in range(2)
            ],
            axis=0,
        )

    right = (r, lax.rem(c + 1, COLS))
    for g in range(GROUPS):
        pltpu.make_async_remote_copy(
            x_ref.at[most], held.at[most], there_send, there_recv.at[g], device_id=right, device_id_type=MESH
        ).wait_recv()
        matrix = rows_of(g)
        grams[g, c] = product(matrix, matrix, 1)
        for step in range(1, COLS):
            pltpu.make_async_remote_copy(
                grams.at[g, c], grams.at[g, c], gram_send, gram_recv.at[g],
                device_id=(r, lax.rem(c + step, COLS)), device_id_type=MESH,
            ).start()
        pltpu.make_async_remote_copy(
            grams.at[g, pl.ds(0, COLS - 1)], grams.at[g, pl.ds(0, COLS - 1)], gram_send, gram_recv.at[g],
            device_id=right, device_id_type=MESH,
        ).wait_recv()
        gram = (grams[g, 0] + grams[g, 1]) + (grams[g, 2] + grams[g, 3])
        scale = lax.rsqrt(jnp.sum(jnp.where(diagonal, gram, 0.0), axis=(0, 1), keepdims=True) + 1e-06)
        gram = (gram * scale) * scale
        total = None
        for step in range(ITERS):
            mixed = -4.775 * gram + 2.0315 * product(gram, gram)
            if step == 0:
                total = jnp.where(diagonal, 3.4445, 0.0) + mixed
            else:
                total = 3.4445 * total + product(mixed, total)
            if step < ITERS - 1:
                gram = 3.4445 * gram + product(mixed, gram)
                gram = 3.4445 * gram + product(mixed, gram)
        result = product(total * scale, matrix)
        for s in range(2):
            for j in range(UNIT // 2):
                done[pl.ds(g * WHOLE + j * 2 + s, half, stride=UNIT), :] = result[
                    s * half : (s + 1) * half, j * LANES : (j + 1) * LANES
                ]

        for_all(
            lambda p: pltpu.make_async_remote_copy(
                done.at[unit((g * ROWS + p) * UNIT)],
                back_ref.at[unit((g * ROWS + r) * UNIT)],
                back_send, back_recv.at[g],
                device_id=(p, c), device_id_type=MESH,
            ).start(),
            g == GROUPS - 1,
        )
        own = unit((g * ROWS + r) * UNIT)
        back_ref[own, :] = done[own, :]

    weights.wait()
    for g in range(GROUPS):
        pltpu.make_async_remote_copy(
            x_ref.at[most], back_ref.at[most], there_send, back_recv.at[g], device_id=right, device_id_type=MESH
        ).wait_recv()
        back_ref[chunk(g), :] = (1.0 - learn_rate * decay_rate) * w_buf[chunk(g), :] - learn_rate * back_ref[chunk(g), :]

    whole = pl.ds(0, (ROWS - 1) * UNIT * GROUPS)
    pltpu.make_async_remote_copy(
        x_ref.at[whole], held.at[whole], there_send, there_recv.at[0], device_id=right, device_id_type=MESH
    ).wait_send()
    pltpu.make_async_remote_copy(
        done.at[whole], back_ref.at[whole], back_send, back_recv.at[0], device_id=right, device_id_type=MESH
    ).wait_send()
    sent = grams.at[pl.ds(0, COLS - 1)]
    pltpu.make_async_remote_copy(
        sent, sent, gram_send, gram_recv.at[0], device_id=right, device_id_type=MESH
    ).wait_send()


def write(weights, momentum, weights_out, momentum_out, sems):
    copies = [
        pltpu.make_async_copy(weights, weights_out, sems.at[0]),
        pltpu.make_async_copy(momentum, momentum_out, sems.at[1]),
    ]
    for copy in copies:
        copy.start()
    for copy in copies:
        copy.wait()


def flat(x):
    return x.reshape(256, 2, 8, 128).transpose(0, 2, 1, 3).reshape(4096, 128)


def unflat(x):
    return x.reshape(256, 8, 2, 128).transpose(0, 2, 1, 3).reshape(256, 2, 1024)


def local(gradients, momentum, weights):
    shape = (ROWS * GROUPS * UNIT, LANES)
    new_weights, new_momentum = pl.pallas_call(
        kernel,
        name="orthogonal",
        out_shape=[jax.ShapeDtypeStruct(shape, jnp.float32)] * 2,
        in_specs=[pl.BlockSpec(memory_space=pltpu.HBM)] * 3,
        out_specs=[pl.BlockSpec(memory_space=pltpu.VMEM)] * 2,
        scratch_shapes=[
            pltpu.VMEM(shape, jnp.float32),
            pltpu.VMEM((GROUPS, COLS, SIDE, SIDE), jnp.float32),
            pltpu.VMEM(shape, jnp.float32),
            pltpu.VMEM(shape, jnp.float32),
            pltpu.VMEM(shape, jnp.float32),
            pltpu.VMEM(shape, jnp.float32),
            pltpu.SemaphoreType.REGULAR((3,)),
            pltpu.SemaphoreType.DMA((2, GROUPS)),
            pltpu.SemaphoreType.DMA,
            pltpu.SemaphoreType.DMA,
            pltpu.SemaphoreType.DMA((GROUPS,)),
            pltpu.SemaphoreType.DMA,
            pltpu.SemaphoreType.DMA((GROUPS,)),
            pltpu.SemaphoreType.DMA,
            pltpu.SemaphoreType.DMA((GROUPS,)),
        ],
        compiler_params=pltpu.CompilerParams(collective_id=0, has_side_effects=True, vmem_limit_bytes=VMEM_LIMIT),
    )(*(pltpu.with_memory_space_constraint(flat(x), pltpu.HBM) for x in (gradients, momentum, weights)))
    new_weights, new_momentum = pl.pallas_call(
        write,
        name="write",
        out_shape=[jax.ShapeDtypeStruct(shape, jnp.float32)] * 2,
        in_specs=[pl.BlockSpec(memory_space=pltpu.VMEM)] * 2,
        out_specs=[pl.BlockSpec(memory_space=pltpu.HBM)] * 2,
        scratch_shapes=[pltpu.SemaphoreType.DMA((2,))],
        compiler_params=pltpu.CompilerParams(vmem_limit_bytes=8 * 1024 * 1024),
    )(new_weights, new_momentum)
    return (unflat(new_weights), unflat(new_momentum))


def solution(mesh):
    placed = (P(None, "rows", "cols"), P(None, "rows", "cols"), P(None, "rows", "cols"))
    return jax.shard_map(
        local,
        mesh=mesh,
        in_specs=placed,
        out_specs=(P(None, "rows", "cols"), P(None, "rows", "cols")),
        check_vma=False,
    )
```
